32 devices in a mesh: ctx: 8 (over y, x, core), dp: 4 (over z).
Axes of the slice: x: 2, y: 2, z: 4, core: 2. Of those that a mesh axis runs over, the one named last changes fastest.
Arguments:
- query_previous: bfloat16 [4, 1024, 2048], P('dp', 'ctx'), may hold values from -240 to 240
- key_previous: bfloat16 [4, 1024, 512], P('dp', 'ctx'), may hold values from -6 to 6
- value_previous: bfloat16 [4, 1024, 512], P('dp', 'ctx'), may hold values from -6 to 6
- span_order: int32 [16], replicated, may hold values from 0 to 15, each once
- resid: bfloat16 [4, 1024, 4096], P('dp', 'ctx'), may hold values from -6 to 6
- grad_norm: bfloat16 [4, 1024, 4096], P('dp', 'ctx'), may hold values from -3 to 3
- gain: float32 [4096], replicated, may hold values from 0.1 to 1.9
Outputs:
- out_prev: bfloat16 [4, 1024, 2048], P('dp', 'ctx')
- lse_prev: float32 [4, 16, 1024], P('dp', None, 'ctx')
- resid_grad: bfloat16 [4, 1024, 4096], P('dp', 'ctx')
- gain_grad: float32 [4096], replicated
The draws below stay inside these ranges and needn't reach their ends.
Inputs may be any that keep to these rules, and one draw needn't show every extreme that they name: span_order names each of the 16 spans once; rows c * 64 to (c + 1) * 64 - 1 of a sequence's arrays hold span span_order[c].
All inputs are finite; a program needn't handle non-finite values.
Results may differ from the reference program's by a relative error of at most 0.0055.
Values may be sent and summed in bfloat16 or wider, within the bound.
No kernel may reach another device: no remote copies, remote signals or barrier semaphores. Data moves between devices by JAX's collectives and lax.ppermute only.
A program may use at most 64 MiB of HBM per device.

```python
import math
import jax
import jax.numpy as jnp
from jax import lax

D = 4096
QUERY_HEADS = 16
KEY_VALUE_HEADS = 4
HEAD_WIDTH = 128
TOK_DEV = 128
SPANS = 16
SEQUENCE_TOKENS = 1024
SEQUENCE_COUNT = 4
N_CTX = 8


def draw_query_previous(key, part):
    base = jax.random.truncated_normal(key, -6.0, 6.0, (SEQUENCE_COUNT, SEQUENCE_TOKENS, QUERY_HEADS * HEAD_WIDTH), jnp.float32)
    return base.astype(jnp.bfloat16)


def block_levels(own_key, extent, split, low, top_value):
    factor_of, own = 1.0, jax.random.fold_in(own_key, 6)
    for dim, blocks in split:
        steps = jnp.exp(jax.random.uniform(jax.random.fold_in(own, dim), (blocks,), jnp.float32, low / len(split), top_value / len(split)))
        factor_of = factor_of * jnp.repeat(steps, extent[dim] // blocks).reshape([-1 if axis == dim else 1 for axis in range(len(extent))])
    return factor_of


def scatter_about(stream_key, dims, deviation, limit, cuts=(), kind=jnp.bfloat16):
    result = jax.random.normal(stream_key, dims, jnp.float32) * deviation
    if len(cuts) > 0:
        result = block_levels(stream_key, dims, cuts, -0.22, 0.18) * result
    return jnp.clip(result, min=-limit, max=limit).astype(kind)


def setup_inputs(seed: int = 0) -> dict:
    key_list = jax.random.split(jax.random.key(seed), 8)
    return {
        "query_previous": draw_query_previous(jax.random.fold_in(key_list[7], 71), 0),
        "key_previous": scatter_about(key_list[1], (SEQUENCE_COUNT, SEQUENCE_TOKENS, KEY_VALUE_HEADS * HEAD_WIDTH), 1.0, 6.0, ((0, 4), (1, 8))),
        "value_previous": scatter_about(key_list[2], (SEQUENCE_COUNT, SEQUENCE_TOKENS, KEY_VALUE_HEADS * HEAD_WIDTH), 1.0, 6.0, ((0, 4), (1, 8))),
        "span_order": jax.random.permutation(key_list[3], SPANS).astype(jnp.int32),
        "resid": scatter_about(key_list[4], (SEQUENCE_COUNT, SEQUENCE_TOKENS, D), 1.0, 6.0, ((0, 4), (1, 8))),
        "grad_norm": scatter_about(key_list[5], (SEQUENCE_COUNT, SEQUENCE_TOKENS, D), 0.5, 3.0, ((0, 4), (1, 8))),
        "gain": jnp.clip(1.0 + 0.18 * jax.random.normal(key_list[6], (D,), jnp.float32), 0.1, 1.9),
    }


def positions(span_order):
    half = TOK_DEV // 2
    index = jnp.arange(TOK_DEV * N_CTX, dtype=jnp.int32)
    return (span_order[index // half] * half + index % half).astype(jnp.int32)

def attend_rows(query_rows, q_positions, key_rows, value_rows, k_positions):
    query_group = QUERY_HEADS // KEY_VALUE_HEADS
    tally_count = query_rows.shape[0]
    query_four_axes = query_rows.astype(jnp.float32).reshape(tally_count, KEY_VALUE_HEADS, query_group, HEAD_WIDTH)
    key_three_axes = key_rows.astype(jnp.float32).reshape(-1, KEY_VALUE_HEADS, HEAD_WIDTH)
    value_three_axes = value_rows.astype(jnp.float32).reshape(-1, KEY_VALUE_HEADS, HEAD_WIDTH)
    scores = jnp.einsum('rkgd,skd->kgrs', query_four_axes, key_three_axes) * HEAD_WIDTH ** (-0.5)
    mask = (k_positions[None, :] <= q_positions[:, None])[None, None]
    scores = jnp.where(mask, scores, -1e+30)
    top = lax.optimization_barrier(jnp.max(scores, axis=-1))
    weights = jnp.where(mask, jnp.exp(scores - top[..., None]), 0.0)
    total = lax.optimization_barrier(jnp.sum(weights, axis=-1))
    probs = lax.optimization_barrier(weights.astype(jnp.bfloat16)).astype(jnp.float32)
    summed = jnp.einsum('kgrs,skd->rkgd', probs, value_three_axes)
    output = summed / jnp.transpose(total, (2, 0, 1))[..., None]
    lse = (top + jnp.log(total)).reshape(QUERY_HEADS, tally_count)
    return (output.reshape(tally_count, QUERY_HEADS * HEAD_WIDTH).astype(jnp.bfloat16), lse)

def reference(query_previous, key_previous, value_previous, span_order, resid, grad_norm, gain):
    length = TOK_DEV * N_CTX
    pos = positions(span_order)
    block = math.gcd(length, 512)
    blocks = length // block

    def one_sequence(items):
        query_rows, key_rows, value_rows = items
        q_blocks = query_rows.reshape(blocks, block, QUERY_HEADS * HEAD_WIDTH)
        p_blocks = pos.reshape(blocks, block)
        outs, lses = lax.map(lambda pair: attend_rows(pair[0], pair[1], key_rows, value_rows, pos), (q_blocks, p_blocks))
        lse = jnp.transpose(lses, (1, 0, 2)).reshape(QUERY_HEADS, length)
        return (outs.reshape(length, QUERY_HEADS * HEAD_WIDTH), lse)
    out_prev, lse_prev = lax.map(one_sequence, (query_previous, key_previous, value_previous))
    resid_f = resid.astype(jnp.float32)
    grad_f = grad_norm.astype(jnp.float32)
    inv_rms = 1.0 / jnp.sqrt(lax.optimization_barrier(jnp.mean(resid_f * resid_f, axis=-1, keepdims=True)) + 1e-05)
    normed = resid_f * inv_rms
    gain_grad = lax.optimization_barrier(jnp.sum(grad_f * normed, axis=(0, 1)))
    scaled = gain[None, None, :] * grad_f
    resid_grad = ((scaled - normed * lax.optimization_barrier(jnp.mean(scaled * normed, axis=-1, keepdims=True))) * inv_rms).astype(jnp.bfloat16)
    return (out_prev, lse_prev, resid_grad, gain_grad)
```

```python
import functools
import math

import jax
import jax.numpy as jnp
from jax import lax
from jax.experimental import pallas as pl
from jax.experimental.pallas import tpu as pltpu
from jax.sharding import PartitionSpec as P

QUERY_HEADS = 16
KEY_VALUE_HEADS = 4
HEAD_WIDTH = 128
GROUP = QUERY_HEADS // KEY_VALUE_HEADS
MASKED = -1e30
LOG2E = math.log2(math.e)
LN2 = math.log(2.0)


VMEM = pl.BlockSpec(memory_space=pltpu.VMEM)
SMEM = pl.BlockSpec(memory_space=pltpu.SMEM)


def norm_kernel(x_ref, g_ref, gain_ref, out_ref, part_ref, sums):
    rows, width = x_ref.shape
    step = 16
    cut = 512
    sums[...] = jnp.zeros_like(sums)

    def body(i, unused):
        r = pl.ds(pl.multiple_of(i * step, step), step)
        square = jnp.zeros((step, 128), jnp.float32)
        for c in range(0, width, 128):
            x = x_ref[r, c : c + 128].astype(jnp.float32)
            square = square + x * x
        inv = 1.0 / jnp.sqrt(jnp.sum(square, axis=-1, keepdims=True) / width + 1e-05)
        dot = jnp.zeros((step, 128), jnp.float32)
        for c in range(0, width, 128):
            x = x_ref[r, c : c + 128].astype(jnp.float32)
            g = g_ref[r, c : c + 128].astype(jnp.float32)
            term = g * (x * inv)
            sums[:, c : c + 128] += term[:8] + term[8:]
            dot = dot + term * gain_ref[:, c : c + 128]
        mean = jnp.sum(dot, axis=-1, keepdims=True) / width
        back = mean * inv * inv
        for c in range(0, width, 128):
            x = x_ref[r, c : c + 128].astype(jnp.float32)
            g = g_ref[r, c : c + 128].astype(jnp.float32)
            out_ref[r, c : c + 128] = (gain_ref[:, c : c + 128] * g * inv - x * back).astype(
                jnp.bfloat16
            )
        return unused

    lax.fori_loop(0, rows // step, body, 0)
    for c in range(0, width, cut):
        part_ref[:, c : c + cut] = jnp.sum(sums[:, c : c + cut], axis=0, keepdims=True)


def norm_backward(resid, grad_norm, gain):
    rows, width = resid.shape
    return pl.pallas_call(
        norm_kernel,
        out_shape=(
            jax.ShapeDtypeStruct((rows, width), jnp.bfloat16),
            jax.ShapeDtypeStruct((1, width), jnp.float32),
        ),
        in_specs=[VMEM] * 3,
        out_specs=(VMEM, VMEM),
        scratch_shapes=[pltpu.VMEM((8, width), jnp.float32)],
        cost_estimate=pl.CostEstimate(
            flops=16 * rows * width, bytes_accessed=6 * rows * width, transcendentals=0
        ),
        name="norm_backward",
    )(resid, grad_norm, gain[None])


def positions(spans_ref, owner, spans, half, index):
    slot = index // half
    chosen = jnp.zeros_like(index)
    for s in range(spans):
        chosen = jnp.where(slot == s, spans_ref[owner * spans + s], chosen)
    return chosen * half + index % half


def attend_kernel(first, last, offsets, spans, spans_ref, q_ref, *refs):
    n = len(offsets)
    k_refs, v_refs, refs = refs[:n], refs[n : 2 * n], refs[2 * n :]
    if not first:
        (top_in, sum_in, acc_in), refs = refs[:3], refs[3:]
    if last:
        out_ref, lse_ref = refs
    else:
        top_out, sum_out, acc_out = refs
    rows = q_ref.shape[0]
    half = rows // spans
    me = lax.axis_index("ctx")
    shape = (rows, rows)
    q_pos = positions(spans_ref, me, spans, half, lax.broadcasted_iota(jnp.int32, shape, 0))
    biases = []
    for d in offsets:
        k_pos = positions(
            spans_ref, me ^ d, spans, half, lax.broadcasted_iota(jnp.int32, shape, 1)
        )
        biases.append(jnp.where(k_pos <= q_pos, 0.0, MASKED))
    bias = jnp.concatenate(biases, axis=1)
    bias = jnp.concatenate([bias] * GROUP, axis=0)
    ones = jnp.ones((n * rows, HEAD_WIDTH), jnp.bfloat16)
    lane = lax.broadcasted_iota(jnp.int32, (rows, HEAD_WIDTH), 1)
    lse = jnp.zeros((rows, HEAD_WIDTH), jnp.float32)
    for h in range(KEY_VALUE_HEADS):
        cols = slice(h * HEAD_WIDTH, (h + 1) * HEAD_WIDTH)
        q = jnp.concatenate(
            [
                q_ref[:, (h * GROUP + j) * HEAD_WIDTH : (h * GROUP + j + 1) * HEAD_WIDTH]
                for j in range(GROUP)
            ],
            axis=0,
        )
        k = jnp.concatenate([ref[:, cols] for ref in k_refs], axis=0)
        v = jnp.concatenate([ref[:, cols] for ref in v_refs], axis=0)
        v = jnp.concatenate([v, ones], axis=1)
        scores = lax.dot_general(
            q, k, (((1,), (1,)), ((), ())), preferred_element_type=jnp.float32
        )
        scores = scores * (LOG2E * HEAD_WIDTH ** (-0.5)) + bias
        top = jnp.max(scores, axis=-1, keepdims=True)
        band = slice(h * GROUP * rows, (h + 1) * GROUP * rows)
        if not first:
            old = top_in[band, :]
            top = jnp.maximum(old, top)
            factor = jnp.exp2(old - top)
            weights = jnp.exp2(scores - top[:, :1])
        else:
            weights = jnp.exp2(scores - top)
            top = jnp.broadcast_to(top, (GROUP * rows, HEAD_WIDTH))
        added = jnp.dot(weights.astype(jnp.bfloat16), v, preferred_element_type=jnp.float32)
        acc, total = added[:, :HEAD_WIDTH], added[:, HEAD_WIDTH:]
        if not first:
            acc = acc + acc_in[band, :] * factor
            total = total + sum_in[band, :] * factor
        if not last:
            top_out[band, :] = top
            sum_out[band, :] = total
            acc_out[band, :] = acc
        else:
            result = (acc / total).astype(jnp.bfloat16)
            logs = (top + jnp.log2(total)) * LN2
            for j in range(GROUP):
                head = h * GROUP + j
                part = slice(j * rows, (j + 1) * rows)
                out_ref[:, head * HEAD_WIDTH : (head + 1) * HEAD_WIDTH] = result[part]
                lse = jnp.where(lane == head, logs[part], lse)
    if last:
        lse_ref[...] = jnp.transpose(lse)[:QUERY_HEADS]


def attend(offsets, spans, span_order, query, keys, values, state, last):
    rows = query.shape[0]
    tall = QUERY_HEADS * rows
    first = state is None
    if last:
        out_shape = (
            jax.ShapeDtypeStruct(query.shape, jnp.bfloat16),
            jax.ShapeDtypeStruct((QUERY_HEADS, rows), jnp.float32),
        )
    else:
        out_shape = (jax.ShapeDtypeStruct((tall, HEAD_WIDTH), jnp.float32),) * 3
    operands = (span_order, query, *keys, *values) + (() if first else state)
    return pl.pallas_call(
        functools.partial(attend_kernel, first, last, offsets, spans),
        out_shape=out_shape,
        in_specs=[SMEM] + [VMEM] * (len(operands) - 1),
        out_specs=(VMEM,) * len(out_shape),
        cost_estimate=pl.CostEstimate(
            flops=4 * tall * HEAD_WIDTH * rows * len(offsets),
            bytes_accessed=4 * tall * HEAD_WIDTH,
            transcendentals=tall * rows * len(offsets),
        ),
        name="attend_" + "_".join(str(d) for d in offsets),
    )(*operands)


def send(x, axis, size, distance):
    return lax.ppermute(x, axis, [(i, i ^ distance) for i in range(size)])


def all_sum(part, n_ctx, n_dp):
    if n_dp & (n_dp - 1):
        part = lax.psum(part, "dp")
    else:
        step = 1
        while step < n_dp:
            part = part + send(part, "dp", n_dp, step)
            step *= 2
    step = 1
    while step < n_ctx:
        part = part + send(part, "ctx", n_ctx, step)
        step *= 2
    return part


def per_device(n_ctx, n_dp, query, key, value, span_order, resid, grad_norm, gain):
    query, key, value = query[0], key[0], value[0]
    spans = span_order.shape[0] // n_ctx
    far = {}
    for d in range(2, n_ctx, 2):
        far[d] = (send(key, "ctx", n_ctx, d), send(value, "ctx", n_ctx, d))
    near = (send(key, "ctx", n_ctx, 1), send(value, "ctx", n_ctx, 1))
    resid_grad, part = norm_backward(resid[0], grad_norm[0], gain)
    gain_grad = all_sum(part, n_ctx, n_dp)
    state = attend(
        (0, 1), spans, span_order, query, (key, near[0]), (value, near[1]), None, False
    )
    for d in range(2, n_ctx, 2):
        k, v = far[d]
        passed = (send(k, "ctx", n_ctx, 1), send(v, "ctx", n_ctx, 1))
        state = attend(
            (d, d + 1),
            spans,
            span_order,
            query,
            (k, passed[0]),
            (v, passed[1]),
            state,
            d + 2 >= n_ctx,
        )
    out, lse = state
    return (out[None], lse[None], resid_grad[None], gain_grad[0])


def solution(mesh):
    n_ctx, n_dp = mesh.shape["ctx"], mesh.shape["dp"]
    return jax.shard_map(
        functools.partial(per_device, n_ctx, n_dp),
        mesh=mesh,
        in_specs=(
            P("dp", "ctx", None),
            P("dp", "ctx", None),
            P("dp", "ctx", None),
            P(),
            P("dp", "ctx", None),
            P("dp", "ctx", None),
            P(),
        ),
        out_specs=(P("dp", "ctx", None), P("dp", None, "ctx"), P("dp", "ctx", None), P()),
        check_vma=False,
    )
```
